128 devices in a mesh: pool: 4 (over y), tp: 32 (over x, z, core).
Axes of the slice: x: 4, y: 4, z: 4, core: 2. Of those that a mesh axis runs over, the one named last changes fastest.
Arguments:
- prompt_states: bfloat16 [3584, 8192], P(('pool', 'tp')), may hold values from -32 to 32
- stretch_slot: int32 [3584], replicated, may hold values from 0 to 255, as said below
- cache_length: int32 [256], P(('pool', 'tp')), may hold values from 0 to 512, as said below
- cache_keys: bfloat16 [256, 512, 1024], P(('pool', 'tp')), may hold values from -64 to 64
- cache_values: bfloat16 [256, 512, 1024], P(('pool', 'tp')), may hold values from -6 to 6
- step_states: bfloat16 [4, 256, 8192], P(None, ('pool', 'tp')), may hold values from -6 to 6
- query_weight: bfloat16 [8192, 8192], P(None, 'tp'), may hold values from -0.0625 to 0.0625
- key_weight: bfloat16 [8192, 1024], P(None, 'tp'), may hold values from -0.0625 to 0.0625
- value_weight: bfloat16 [8192, 1024], P(None, 'tp'), may hold values from -0.0625 to 0.0625
Outputs:
- prompt_out: bfloat16 [3584, 8192], P('pool', 'tp')
- step_out: bfloat16 [4, 256, 8192], P(None, ('pool', 'tp'))
The draws below stay inside these ranges and needn't reach their ends.
Inputs may be any that keep to these rules, and one draw needn't show every extreme that they name: `stretch_slot`: each group's 896 tokens are whole prompts of 24 to 32 tokens in consecutive runs; no slot is named by two prompts; some prompt has 32 tokens. `cache_length`: 0 for every slot that stretch_slot names, 1 or more for the others; some slot has 512.
All inputs are finite; a program needn't handle non-finite values.
Results may differ from the reference program's by a relative error of at most 0.0094.
Values may be sent and summed in bfloat16 or wider, within the bound.
No kernel may reach another device: no remote copies, remote signals or barrier semaphores. Data moves between devices by JAX's collectives and lax.ppermute only.
A program may use at most 128 MiB of HBM per device.

```python
import math
import jax
import jax.numpy as jnp
from jax import lax

D = 8192
HEADS = 64
KV_HEADS = 8
HEAD = 128
PMAX = 32
CL = 512
STEPS = 4
PT = 896
R = 256
N_POOL = 4


def prompt_sizes(key):
    prompt_count = PT // (7 * PMAX // 8)
    lowest = 3 * PMAX // 4
    key_walk, key_group, key_index, key_donor = jax.random.split(key, 4)
    groups = jnp.arange(N_POOL, dtype=jnp.int32)
    places = jnp.arange(prompt_count, dtype=jnp.int32)
    sizing = jnp.full((N_POOL, prompt_count), 7 * PMAX // 8, jnp.int32)

    def wander(turn_index, current):
        endpoints = jax.random.randint(jax.random.fold_in(key_walk, turn_index), (2, N_POOL), 0, prompt_count)
        source = endpoints[0]
        target = endpoints[1]
        movable = (source != target) & (current[groups, source] > lowest) & (current[groups, target] < PMAX)
        amount = movable.astype(jnp.int32)
        current = current.at[groups, source].add(-amount)
        return current.at[groups, target].add(amount)
    sizing = lax.fori_loop(0, 16 * prompt_count, wander, sizing)
    chosen_group = jax.random.randint(key_group, (), 0, N_POOL)
    chosen = jax.random.randint(key_index, (), 0, prompt_count)

    def raise_chosen(turn_index, current):
        scores = jax.random.permutation(jax.random.fold_in(key_donor, turn_index), prompt_count).astype(jnp.int32)
        group_row = current[chosen_group]
        eligible = (places != chosen) & (group_row > lowest)
        donor_index = jnp.argmax(jnp.where(eligible, scores, -1))
        amount = (group_row[chosen] < PMAX).astype(jnp.int32)
        group_row = group_row.at[donor_index].add(-amount).at[chosen].add(amount)
        return current.at[chosen_group].set(group_row)
    return lax.fori_loop(0, PMAX - lowest, raise_chosen, sizing)


def arrange(key):
    drawn = jax.random.fold_in(key, 7)
    key_sizes, key_order, key_left, key_right = jax.random.split(drawn, 4)
    sizing = prompt_sizes(key_sizes)
    prompt_count = sizing.shape[1]
    ordering = jax.random.permutation(key_order, R)
    newcomers = N_POOL * prompt_count
    owners = ordering[:newcomers].reshape(N_POOL, prompt_count)
    endings = jnp.cumsum(sizing, axis=1)
    places = jnp.arange(PT)
    which_prompt = jnp.sum(places[None, :, None] >= endings[:, None, :], axis=2)
    stretch_slot = jnp.take_along_axis(owners, which_prompt, axis=1).reshape(N_POOL * PT)
    left_draw = jax.random.randint(key_left, (R,), 0, CL + 1)
    right_draw = jax.random.randint(key_right, (R,), 0, CL + 1)
    lengths = jnp.minimum(1 + left_draw * right_draw // CL, CL)
    lengths = lengths.at[owners.reshape(-1)].set(0)
    lengths = lengths.at[ordering[newcomers]].set(CL)
    return (stretch_slot.astype(jnp.int32), lengths.astype(jnp.int32))


def draw_stretch_slot(key, part):
    return arrange(key)[0]


def draw_cache_length(key, part):
    return arrange(key)[1]


def draw_prompt_states(key, part):
    shape = (N_POOL * PT, D)
    drawn = jax.random.normal(key, shape, jnp.float32)
    return jnp.clip(drawn, -32.0, 32.0).astype(jnp.bfloat16)


def draw_cache_keys(key, part):
    width = KV_HEADS * HEAD
    drawn = jnp.clip(jax.random.normal(key, (R, CL, width), jnp.float32), -6.0, 6.0)
    return drawn.astype(jnp.bfloat16)


def block_scale(key, shape, shards, smallest, largest):
    loudness = 1.0
    for axis_at, shards_of in shards:
        steps = jax.random.uniform(jax.random.fold_in(jax.random.fold_in(key, 6), axis_at), (shards_of,), jnp.float32, smallest / len(shards), largest / len(shards))
        loudness = loudness * jnp.repeat(jnp.exp(steps), shape[axis_at] // shards_of).reshape((-1,) + (1,) * (len(shape) - 1 - axis_at))
    return loudness


def centred(key, shape, scale, limit, pieces=(), held_as=jnp.bfloat16):
    loudness = block_scale(key, shape, pieces, -0.22, 0.18) if pieces else 1.0
    result = jax.random.normal(key, shape, jnp.float32) * scale * loudness
    return jnp.minimum(jnp.maximum(result, -limit), limit).astype(held_as)


def setup_inputs(seed: int = 0) -> dict:
    key_of = jax.random.split(jax.random.key(seed), 10)
    prompt_states = draw_prompt_states(jax.random.fold_in(key_of[9], 71), 0)
    stretch_slot = draw_stretch_slot(jax.random.fold_in(key_of[9], 71), 0)
    cache_length = draw_cache_length(jax.random.fold_in(key_of[9], 71), 0)
    cache_keys = draw_cache_keys(jax.random.fold_in(key_of[9], 71), 0)
    cache_values = centred(key_of[4], (R, CL, KV_HEADS * HEAD), 1.0, 6.0, ((0, 128),))
    step_states = centred(key_of[5], (STEPS, R, D), 1.0, 6.0, ((1, 128),))
    query_weight = centred(key_of[6], (D, HEADS * HEAD), D ** -0.5, 0.0625, ((1, 32),))
    key_weight = centred(key_of[7], (D, KV_HEADS * HEAD), D ** -0.5, 0.0625, ((1, 32),))
    value_weight = centred(key_of[8], (D, KV_HEADS * HEAD), D ** -0.5, 0.0625, ((1, 32),))
    return dict(prompt_states=prompt_states, stretch_slot=stretch_slot, cache_length=cache_length, cache_keys=cache_keys, cache_values=cache_values, step_states=step_states, query_weight=query_weight, key_weight=key_weight, value_weight=value_weight)


rope_base = 500000.0
negative_fill = -1e+30

def frequencies(half):
    indices = jnp.arange(half, dtype=jnp.float32)
    inverse = rope_base ** (-2.0 * indices / (2.0 * half))
    wavelength = 2.0 * math.pi / inverse
    blend = (8192.0 / wavelength - 1.0) / 3.0
    middle = (1.0 - blend) * inverse / 8.0 + blend * inverse
    scaled = jnp.where(wavelength > 8192.0, inverse / 8.0, inverse)
    inside = (wavelength >= 2048.0) & (wavelength <= 8192.0)
    return jnp.where(inside, middle, scaled)

def rotate(values, positions):
    half = values.shape[-1] // 2
    angles = positions.astype(jnp.float32)[..., None, None] * frequencies(half)
    cosine = jnp.cos(angles)
    sine = jnp.sin(angles)
    upper = values[..., :half].astype(jnp.float32)
    lower = values[..., half:].astype(jnp.float32)
    return jnp.concatenate([upper * cosine - lower * sine, lower * cosine + upper * sine], axis=-1)

def run_positions(slots, span):
    indices = jnp.arange(slots.shape[0], dtype=jnp.int32)
    previous = jnp.concatenate([slots[:1] - 1, slots[:-1]])
    opening = (slots != previous) | (indices % span == 0)
    starts = lax.cummax(jnp.where(opening, indices, 0), axis=0)
    return indices - starts

def normalize(scores):
    peak = lax.optimization_barrier(jnp.max(scores, axis=-1, keepdims=True))
    raised = jnp.exp(scores - peak)
    return (raised / lax.optimization_barrier(jnp.sum(raised, axis=-1, keepdims=True))).astype(jnp.bfloat16)

def prompt_group(queries, key_rows, value_rows, slots):
    row_count = queries.shape[0]
    grouped = queries.reshape(row_count, KV_HEADS, HEADS // KV_HEADS, HEAD).astype(jnp.float32)
    scores = jnp.einsum('qkgd,lkd->kgql', grouped, key_rows.astype(jnp.float32)) * (1.0 / math.sqrt(HEAD))
    indices = jnp.arange(row_count, dtype=jnp.int32)
    allowed = (slots[:, None] == slots[None, :]) & (indices[None, :] <= indices[:, None])
    weights = normalize(jnp.where(allowed, scores, negative_fill))
    context = jnp.einsum('kgql,lkd->qkgd', weights.astype(jnp.float32), value_rows.astype(jnp.float32))
    return context.reshape(row_count, HEADS * HEAD).astype(jnp.bfloat16)

def decode_slot(items):
    queries, cache_k, cache_v, prompt_k, prompt_v, recent_k, recent_v, valid = items
    key_all = jnp.concatenate([cache_k, prompt_k, recent_k], axis=0)
    value_all = jnp.concatenate([cache_v, prompt_v, recent_v], axis=0)
    key_all = key_all.reshape(key_all.shape[0], KV_HEADS, HEAD).astype(jnp.float32)
    value_all = value_all.reshape(value_all.shape[0], KV_HEADS, HEAD).astype(jnp.float32)
    grouped = queries.reshape(KV_HEADS, HEADS // KV_HEADS, HEAD).astype(jnp.float32)
    scores = jnp.einsum('kgd,lkd->kgl', grouped, key_all) * (1.0 / math.sqrt(HEAD))
    weights = normalize(jnp.where(valid[None, None, :], scores, negative_fill))
    context = jnp.einsum('kgl,lkd->kgd', weights.astype(jnp.float32), value_all)
    return context.reshape(HEADS * HEAD).astype(jnp.bfloat16)

def reference(prompt_states, stretch_slot, cache_length, cache_keys, cache_values, step_states, query_weight, key_weight, value_weight):
    kv_width = KV_HEADS * HEAD
    all_rows = stretch_slot.shape[0]
    query_raw = jnp.dot(prompt_states, query_weight, preferred_element_type=jnp.float32).astype(jnp.bfloat16)
    key_raw = jnp.dot(prompt_states, key_weight, preferred_element_type=jnp.float32).astype(jnp.bfloat16)
    value_rows = jnp.dot(prompt_states, value_weight, preferred_element_type=jnp.float32).astype(jnp.bfloat16)
    positions = run_positions(stretch_slot, PT)
    queries = rotate(query_raw.reshape(all_rows, HEADS, HEAD), positions).astype(jnp.bfloat16)
    key_rows = rotate(key_raw.reshape(all_rows, KV_HEADS, HEAD), positions).astype(jnp.bfloat16)
    value_heads = value_rows.reshape(all_rows, KV_HEADS, HEAD)

    def one_group(group_index):
        anchor = (group_index * PT).astype(jnp.int32)
        return prompt_group(lax.dynamic_slice_in_dim(queries, anchor, PT, 0), lax.dynamic_slice_in_dim(key_rows, anchor, PT, 0), lax.dynamic_slice_in_dim(value_heads, anchor, PT, 0), lax.dynamic_slice_in_dim(stretch_slot, anchor, PT, 0))
    prompt_out = lax.map(one_group, jnp.arange(N_POOL, dtype=jnp.int32)).reshape(all_rows, HEADS * HEAD)
    every_slot = jnp.arange(R, dtype=jnp.int32)
    matches = stretch_slot[None, :] == every_slot[:, None]
    counts = lax.optimization_barrier(jnp.sum(matches, axis=1)).astype(jnp.int32)
    begins = lax.optimization_barrier(jnp.min(jnp.where(matches, jnp.arange(all_rows, dtype=jnp.int32)[None, :], all_rows), axis=1))
    offsets = jnp.arange(PMAX, dtype=jnp.int32)
    row_ids = jnp.clip(begins[:, None] + offsets[None, :], 0, all_rows - 1)
    prompt_keys = jnp.take(key_rows.reshape(all_rows, kv_width), row_ids, axis=0)
    prompt_values = jnp.take(value_rows, row_ids, axis=0)
    recent_keys = jnp.zeros((R, STEPS, kv_width), jnp.bfloat16)
    recent_values = jnp.zeros((R, STEPS, kv_width), jnp.bfloat16)
    cache_live = jnp.arange(CL, dtype=jnp.int32)[None, :] < cache_length[:, None]
    prompt_live = offsets[None, :] < counts[:, None]
    results = []
    for step_index in range(STEPS):
        states = step_states[step_index]
        step_query_raw = jnp.dot(states, query_weight, preferred_element_type=jnp.float32).astype(jnp.bfloat16)
        step_key_raw = jnp.dot(states, key_weight, preferred_element_type=jnp.float32).astype(jnp.bfloat16)
        step_value = jnp.dot(states, value_weight, preferred_element_type=jnp.float32).astype(jnp.bfloat16)
        moment = cache_length + counts + step_index
        step_query = rotate(step_query_raw.reshape(R, HEADS, HEAD), moment).astype(jnp.bfloat16)
        step_key = rotate(step_key_raw.reshape(R, KV_HEADS, HEAD), moment).astype(jnp.bfloat16).reshape(R, kv_width)
        recent_keys = recent_keys.at[:, step_index].set(step_key)
        recent_values = recent_values.at[:, step_index].set(step_value)
        recent_live = jnp.broadcast_to(jnp.arange(STEPS, dtype=jnp.int32)[None, :] <= step_index, (R, STEPS))
        valid = jnp.concatenate([cache_live, prompt_live, recent_live], axis=1)
        results.append(lax.map(decode_slot, (step_query, cache_keys, cache_values, prompt_keys, prompt_values, recent_keys, recent_values, valid)))
    step_out = jnp.stack(results, axis=0)
    return (prompt_out, step_out)
```

```python
import math

import jax
import jax.numpy as jnp
from jax import lax
from jax.experimental import pallas as pl
from jax.experimental.pallas import tpu as pltpu
from jax.sharding import Mesh, PartitionSpec as P

HEADS = 64
KV_HEADS = 8
HEAD = 128
STEPS = 4
RUNS = 40
COMPACT = RUNS * STEPS
X, Z, CORES, POOLS = 4, 4, 2, 4
CHIPS = X * Z
TP = ("x", "z", "core")
ALL = ("pool", "x", "z", "core")
OFFSETS = (0, -1, 1, 2)

rope_base = 500000.0
negative_fill = -1e30
SCALE = 1.0 / math.sqrt(HEAD)


def frequencies(half):
    indices = jnp.arange(half, dtype=jnp.float32)
    inverse = rope_base ** (-2.0 * indices / (2.0 * half))
    wavelength = 2.0 * math.pi / inverse
    blend = (8192.0 / wavelength - 1.0) / 3.0
    middle = (1.0 - blend) * inverse / 8.0 + blend * inverse
    scaled = jnp.where(wavelength > 8192.0, inverse / 8.0, inverse)
    inside = (wavelength >= 2048.0) & (wavelength <= 8192.0)
    return jnp.where(inside, middle, scaled)


def rope_tables(positions):
    freq = jnp.tile(frequencies(HEAD // 2), 2)
    angles = positions.astype(jnp.float32)[:, None] * freq
    sign = jnp.where(jnp.arange(HEAD) < HEAD // 2, -1.0, 1.0)
    return jnp.cos(angles), jnp.sin(angles) * sign


def ring_pairs(ring, shift):
    pairs = []
    for x in range(X):
        for z in range(Z):
            for c in range(CORES):
                along_x = (c == 0) == (ring == 1)
                to_x, to_z = ((x + shift) % X, z) if along_x else (x, (z + shift) % Z)
                pairs.append(((x * Z + z) * CORES + c, (to_x * Z + to_z) * CORES + c))
    return pairs


def hop(value, ring, shift):
    return lax.ppermute(value, TP, ring_pairs(ring, shift))


def both(value, ring):
    return hop(value, ring, 1), hop(value, ring, -1)


def onward(from_left, from_right, ring, cut):
    return jnp.concatenate([hop(from_left[:cut], ring, 1), hop(from_right[cut:], ring, -1)], 0)


def core_swap(value):
    return lax.ppermute(value, "core", [(0, 1), (1, 0)])


def pool_others(value):
    return tuple(
        lax.ppermute(value, "pool", [(j, (j - s) % POOLS) for j in range(POOLS)])
        for s in OFFSETS[1:]
    )


def rotated(value, cosine, sine):
    return value * cosine + pltpu.roll(value, HEAD // 2, 1) * sine


def joined(even, odd):
    even, odd = even.astype(jnp.float32), odd.astype(jnp.float32)
    low = lax.broadcasted_iota(jnp.int32, even.shape, 1) < HEAD // 2
    key = jnp.where(low, even, pltpu.roll(odd, HEAD // 2, 1))
    value = jnp.where(low, pltpu.roll(even, HEAD // 2, 1), odd)
    return key, value.astype(jnp.bfloat16)


def ordered(parity, own, other):
    own, other = own.astype(jnp.float32), other.astype(jnp.float32)
    return jnp.where(parity == 0, own, other), jnp.where(parity == 0, other, own)


def scores_of(queries, keys):
    return (
        lax.dot_general(
            queries, keys, (((1,), (1,)), ((), ())), preferred_element_type=jnp.float32
        )
        * SCALE
    )


def softmax_parts(parts):
    peak = None
    for part in parts:
        top = jnp.max(part, axis=1, keepdims=True)
        peak = top if peak is None else jnp.maximum(peak, top)
    raised = [jnp.exp(part - peak) for part in parts]
    total = sum(jnp.sum(part, axis=1, keepdims=True) for part in raised)
    inverse = 1.0 / total
    return [(part * inverse).astype(jnp.bfloat16) for part in raised]


def times(weights, values):
    return jnp.dot(weights, values, preferred_element_type=jnp.float32)


def whole(*shape):
    return pl.BlockSpec(shape, lambda *_: (0,) * len(shape))


VM = pl.BlockSpec(memory_space=pltpu.VMEM)
SM = pl.BlockSpec(memory_space=pltpu.SMEM)


def assemble(tables, own, received, width):
    rows, columns = received[0].shape[1:]

    def kernel(table, *refs):
        count = len(own)
        mine, theirs = refs[:count], refs[count : 2 * count]
        query, pair, total = refs[2 * count :]
        at = 0
        for ref in mine:
            for k in range(ref.shape[0]):
                total[table[0, at]] = ref[k]
                at += 1
        at = 0
        for ref in theirs:
            for k in range(ref.shape[0]):
                chip = table[1, at]
                added = (total[chip] + ref[k]).astype(jnp.bfloat16)
                query[chip] = added[:, :width]
                pair[chip] = added[:, width:]
                at += 1

    return pl.pallas_call(
        kernel,
        out_shape=(
            jax.ShapeDtypeStruct((CHIPS, rows, width), jnp.bfloat16),
            jax.ShapeDtypeStruct((CHIPS, rows, columns - width), jnp.bfloat16),
        ),
        in_specs=[SM] + [VM] * (2 * len(own)),
        out_specs=(VM, VM),
        scratch_shapes=[pltpu.VMEM((CHIPS, rows, columns), jnp.float32)],
        cost_estimate=pl.CostEstimate(flops=2000000000, bytes_accessed=4000000, transcendentals=0),
    )(tables, *own, *received)


def outgoing(core, prompt_states, step_states):
    tokens, depth = prompt_states.shape
    steps, slots, _ = step_states.shape
    half, head = depth // 2, steps * slots

    def kernel(core_ref, prompt_ref, step_ref, keep, send):
        for out, which in ((keep, core_ref[0]), (send, 1 - core_ref[0])):
            span = pl.ds(pl.multiple_of(which * half, half), half)
            first = [step_ref[k, :, span] for k in range(steps)]
            out[...] = jnp.concatenate(first + [prompt_ref[:, span]], 0)

    shape = jax.ShapeDtypeStruct((head + tokens, half), jnp.bfloat16)
    return pl.pallas_call(
        kernel, out_shape=(shape, shape), in_specs=[SM, VM, VM], out_specs=(VM, VM)
    )(core, prompt_states, step_states)


def paired(core, keep, got, head):
    rows, half = keep.shape

    def kernel(core_ref, keep_ref, got_ref, out):
        keep_value, got_value = keep_ref[...], got_ref[...]
        swap = core_ref[0] == 1
        zero = jnp.where(swap, got_value, keep_value)
        one = jnp.where(swap, keep_value, got_value)
        out[...] = jnp.concatenate([zero[:head], one[:head], zero[head:], one[head:]], 0)

    return pl.pallas_call(
        kernel,
        out_shape=jax.ShapeDtypeStruct((2 * rows, half), jnp.bfloat16),
        in_specs=[SM, VM, VM],
        out_specs=VM,
    )(core, keep, got)


def packed(pieces, far, head):
    rows, half = pieces[0].shape

    def kernel(c0, c1, c2, f0, f1, steps_out, prompts_out):
        for k, ref in enumerate((c0, c1, c2)):
            steps_out[k * head : (k + 1) * head] = ref[:head]
            prompts_out[k * (rows - head) : (k + 1) * (rows - head)] = ref[head:]
        cut = f0.shape[0]
        at = 3 * (rows - head)
        steps_out[3 * head :] = f0[:head]
        prompts_out[at : at + cut - head] = f0[head:]
        prompts_out[at + cut - head :] = f1[...]

    return pl.pallas_call(
        kernel,
        out_shape=(
            jax.ShapeDtypeStruct((4 * head, half), jnp.bfloat16),
            jax.ShapeDtypeStruct((4 * (rows - head), half), jnp.bfloat16),
        ),
        in_specs=[VM] * 5,
        out_specs=(VM, VM),
        cost_estimate=pl.CostEstimate(flops=1000000000, bytes_accessed=4000000, transcendentals=0),
    )(*pieces, *far)


def partial_products(core, pieces, query_weight, query_got, kv_weight):
    rows = sum(p.shape[0] for p in pieces)
    half = pieces[0].shape[1]
    width, narrow = query_weight.shape[1], kv_weight.shape[0]
    steps = 4
    block = half // steps

    def kernel(core_ref, *refs):
        xs = refs[: len(pieces)]
        mine, got, kv, keep, send = refs[len(pieces) :]
        x = xs[0][...] if len(xs) == 1 else jnp.concatenate([r[...] for r in xs], 0)
        kv_part = lax.dot_general(
            x, kv[...], (((1,), (1,)), ((), ())), preferred_element_type=jnp.float32
        )
        keep_part, send_part = times(x, mine[...]), times(x, got[...])

        @pl.when(pl.program_id(0) == 0)
        def _():
            keep[:, :width], send[:, :width] = keep_part, send_part
            keep[:, width:] = kv_part

        @pl.when(pl.program_id(0) > 0)
        def _():
            keep[:, :width] += keep_part
            send[:, :width] += send_part
            keep[:, width:] += kv_part

        @pl.when(pl.program_id(0) == steps - 1)
        def _():
            send[:, width:] = keep[:, width:]

    shape = jax.ShapeDtypeStruct((rows, width + narrow), jnp.float32)
    return pl.pallas_call(
        kernel,
        grid_spec=pltpu.PrefetchScalarGridSpec(
            num_scalar_prefetch=1,
            grid=(steps,),
            in_specs=[pl.BlockSpec((p.shape[0], block), lambda k, c: (0, k)) for p in pieces]
            + [
                pl.BlockSpec((block, width), lambda k, c: (c[0] * steps + k, 0)),
                pl.BlockSpec((block, width), lambda k, c: (k, 0)),
                pl.BlockSpec((narrow, block), lambda k, c: (0, k)),
            ],
            out_specs=[pl.BlockSpec((rows, width + narrow), lambda k, c: (0, 0))] * 2,
        ),
        out_shape=(shape, shape),
        cost_estimate=pl.CostEstimate(
            flops=2 * rows * half * (2 * width + narrow),
            bytes_accessed=2 * rows * half + 2 * half * (2 * width + narrow),
            transcendentals=0,
        ),
    )(core, *pieces, query_weight, query_got, kv_weight)


def cached_attention(arrived, lengths, tables, cache_keys, cache_values):
    slots, extent = cache_keys.shape[:2]
    rows = STEPS * slots
    group = HEADS // KV_HEADS

    def kernel(length, arrived_ref, cosine_ref, sine_ref, key_ref, value_ref, out_ref):
        head = pl.program_id(0)
        cosine, sine = cosine_ref[...], sine_ref[...]
        pieces = []
        for i in range(4):
            for h in range(2):
                raw = arrived_ref[4 * head + i, :, h * HEAD : (h + 1) * HEAD]
                pieces.append(rotated(raw.astype(jnp.float32), cosine, sine))
        queries = jnp.concatenate(pieces, 0).astype(jnp.bfloat16)
        recent_key, recent_value = joined(
            arrived_ref[4 * head, :, 2 * HEAD :], arrived_ref[4 * head + 2, :, 2 * HEAD :]
        )
        recent_key = rotated(recent_key, cosine, sine).astype(jnp.bfloat16)
        total = group * rows
        row = lax.broadcasted_iota(jnp.int32, (total, extent), 0) % rows
        column = lax.broadcasted_iota(jnp.int32, (total, extent), 1)
        parts = []
        for s in range(slots):
            live = (row % slots == s) & (column < length[s])
            parts.append(jnp.where(live, scores_of(queries, key_ref[s]), negative_fill))
        row = lax.broadcasted_iota(jnp.int32, (total, rows), 0) % rows
        column = lax.broadcasted_iota(jnp.int32, (total, rows), 1)
        live = (row % slots == column % slots) & (column // slots <= row // slots)
        parts.append(jnp.where(live, scores_of(queries, recent_key), negative_fill))
        weights = softmax_parts(parts)
        context = times(weights[-1], recent_value)
        for s in range(slots):
            context = context + times(weights[s], value_ref[s])
        for i in range(4):
            for h in range(2):
                at = (i * 2 + h) * rows
                out_ref[i, :, h * HEAD : (h + 1) * HEAD] = context[at : at + rows].astype(
                    jnp.bfloat16
                )

    devices = arrived.shape[0]
    return pl.pallas_call(
        kernel,
        grid=(KV_HEADS,),
        out_shape=jax.ShapeDtypeStruct((devices, rows, 2 * HEAD), jnp.bfloat16),
        in_specs=[
            SM,
            whole(*arrived.shape),
            whole(rows, HEAD),
            whole(rows, HEAD),
            pl.BlockSpec((slots, extent, HEAD), lambda g: (0, 0, g)),
            pl.BlockSpec((slots, extent, HEAD), lambda g: (0, 0, g)),
        ],
        out_specs=pl.BlockSpec((4, rows, 2 * HEAD), lambda g: (g, 0, 0)),
        cost_estimate=pl.CostEstimate(flops=6000000000, bytes_accessed=4500000, transcendentals=0),
    )(lengths, arrived, *tables, cache_keys, cache_values)


def prompt_slot_attention(parity, picks, run_slots, decode_rows, even, odd, tables, run_tables, slot_row):
    def kernel(par, pick, run_slot, d0, d1, d2, d3, own_ref, other_ref, cos, sin, ccos, csin, slot, out):
        compact = None
        each = d0.shape[0]
        for p, ref in enumerate((d0, d1, d2, d3)):
            column = lax.broadcasted_iota(jnp.int32, (COMPACT, each), 1) + p * each
            hot = jnp.where(pick[...] == column, 1.0, 0.0).astype(jnp.bfloat16)
            part = times(hot, ref[...])
            compact = part if compact is None else compact + part
        key, value = joined(*ordered(par[0], own_ref[...], other_ref[...]))
        key = rotated(key, cos[...], sin[...]).astype(jnp.bfloat16)
        recent_key, recent_value = joined(
            *ordered(par[0], compact[:, 2 * HEAD : 3 * HEAD], compact[:, 3 * HEAD :])
        )
        recent_key = rotated(recent_key, ccos[...], csin[...]).astype(jnp.bfloat16)
        live = run_slot[...] == slot[...]
        row = lax.broadcasted_iota(jnp.int32, (COMPACT, COMPACT), 0)
        column = lax.broadcasted_iota(jnp.int32, (COMPACT, COMPACT), 1)
        recent_live = (row % RUNS == column % RUNS) & (column <= row)
        for h in range(2):
            query = compact[:, h * HEAD : (h + 1) * HEAD]
            query = rotated(query, ccos[...], csin[...]).astype(jnp.bfloat16)
            parts = [
                jnp.where(live, scores_of(query, key), negative_fill),
                jnp.where(recent_live, scores_of(query, recent_key), negative_fill),
            ]
            weights = softmax_parts(parts)
            context = times(weights[0], value) + times(weights[1], recent_value)
            out[:, h * HEAD : (h + 1) * HEAD] = context.astype(jnp.bfloat16)

    return pl.pallas_call(
        kernel,
        out_shape=jax.ShapeDtypeStruct((COMPACT, 2 * HEAD), jnp.bfloat16),
        in_specs=[SM] + [VM] * 13,
        out_specs=VM,
        cost_estimate=pl.CostEstimate(flops=6000000000, bytes_accessed=4000000, transcendentals=0),
    )(parity, picks, run_slots, *decode_rows, even, odd, *tables, *run_tables, slot_row)


def prompt_attention(parity, queries, even, odd, tables, slot_column, slot_row):
    count = queries.shape[0]
    block = 128

    def kernel(par, query_ref, own_ref, other_ref, cos, sin, column, row, out):
        key, value = joined(*ordered(par[0], own_ref[...], other_ref[...]))
        key = rotated(key, cos[...], sin[...]).astype(jnp.bfloat16)
        for b in range(count // block):
            here = slice(b * block, (b + 1) * block)
            first = max(0, b - 1) * block
            span = (b + 1) * block - first
            i = lax.broadcasted_iota(jnp.int32, (block, span), 0) + b * block
            j = lax.broadcasted_iota(jnp.int32, (block, span), 1) + first
            live = (column[here, :] == row[:, first : first + span]) & (j <= i)
            for h in range(2):
                query = query_ref[here, h * HEAD : (h + 1) * HEAD].astype(jnp.float32)
                query = rotated(query, cos[here, :], sin[here, :]).astype(jnp.bfloat16)
                scores = scores_of(query, key[first : first + span])
                (weights,) = softmax_parts([jnp.where(live, scores, negative_fill)])
                context = times(weights, value[first : first + span])
                out[here, h * HEAD : (h + 1) * HEAD] = context.astype(jnp.bfloat16)

    return pl.pallas_call(
        kernel,
        out_shape=jax.ShapeDtypeStruct((count, 2 * HEAD), jnp.bfloat16),
        in_specs=[SM] + [VM] * 7,
        out_specs=VM,
        cost_estimate=pl.CostEstimate(flops=4000000000, bytes_accessed=3000000, transcendentals=0),
    )(parity, queries, even, odd, *tables, slot_column, slot_row)


def spread(picks, results):
    rows = CHIPS * CORES * STEPS * 2

    def kernel(pick, r0, r1, r2, r3, out):
        total = None
        for p, ref in enumerate((r0, r1, r2, r3)):
            row = lax.broadcasted_iota(jnp.int32, (rows, COMPACT), 0)
            hot = jnp.where(pick[p : p + 1, :] == row, 1.0, 0.0).astype(jnp.bfloat16)
            part = times(hot, ref[...])
            total = part if total is None else total + part
        out[...] = total.astype(jnp.bfloat16)

    return pl.pallas_call(
        kernel,
        out_shape=jax.ShapeDtypeStruct((rows, 2 * HEAD), jnp.bfloat16),
        in_specs=[VM] * 5,
        out_specs=VM,
        cost_estimate=pl.CostEstimate(flops=1000000000, bytes_accessed=500000, transcendentals=0),
    )(picks, *results)


def merge(cached, prompted, named):
    devices, rows, width = cached.shape

    def kernel(named_ref, cached_ref, prompted_ref, out):
        for k in range(devices):
            out[:, k * width : (k + 1) * width] = jnp.where(
                named_ref[...] > 0, prompted_ref[k].astype(jnp.float32), cached_ref[k].astype(jnp.float32)
            ).astype(jnp.bfloat16)

    return pl.pallas_call(
        kernel,
        out_shape=jax.ShapeDtypeStruct((rows, devices * width), jnp.bfloat16),
        in_specs=[VM] * 3,
        out_specs=VM,
    )(named, cached, prompted)


def row_of(slot, step, per_device):
    return (slot // per_device) * (STEPS * per_device) + step * per_device + slot % per_device


def on_device(
    prompt_states,
    stretch_slot,
    cache_length,
    cache_keys,
    cache_values,
    step_states,
    query_weight,
    key_weight,
    value_weight,
):
    pool, x, z, core = (lax.axis_index(name) for name in ALL)
    device = (x * Z + z) * CORES + core
    first_core = core == 0
    tokens, depth = prompt_states.shape
    half = depth // 2
    per_device = cache_length.shape[0]
    step_rows = STEPS * per_device
    pool_slots = per_device * CHIPS * CORES
    group_tokens = tokens * CHIPS * CORES

    core_ref = core.astype(jnp.int32)[None]
    keep, send = outgoing(core_ref, prompt_states, step_states)
    chunk = paired(core_ref, keep, core_swap(send), step_rows)
    chunk, query_weight, key_weight, value_weight, stretch_slot = lax.optimization_barrier(
        (chunk, query_weight, key_weight, value_weight, stretch_slot)
    )
    steps_each, prompts_each = 2 * step_rows, 2 * tokens

    left, right = both(chunk, 1)

    query_got = core_swap(lax.dynamic_slice_in_dim(query_weight, (1 - core) * half, half, 0))
    narrow = key_weight.shape[1]
    kv_weight = jnp.concatenate([key_weight.T, value_weight.T], 0)
    kv_mine = lax.dynamic_slice_in_dim(kv_weight, core * half, half, 1)
    kv_got = core_swap(lax.dynamic_slice_in_dim(kv_weight, (1 - core) * half, half, 1))
    kv0, kv1 = jnp.where(first_core, kv_mine, kv_got), jnp.where(first_core, kv_got, kv_mine)
    kv_weight = jnp.concatenate([kv0[:narrow], kv1[:narrow], kv0[narrow:], kv1[narrow:]], 0)
    width = query_weight.shape[1]

    def partial_of(pieces, rows):
        kept, sent = partial_products(core_ref, pieces, query_weight, query_got, kv_weight)
        return kept.reshape(-1, rows, kept.shape[1]), core_swap(sent).reshape(
            -1, rows, kept.shape[1]
        )

    cut = 40
    far = hop(left[:cut], 1, 1), hop(right[cut:], 1, -1)
    steps_near, prompts_near = packed((chunk, left, right), far, steps_each)
    steps_left, steps_right = both(steps_near, 2)
    cut = steps_near.shape[0] // 2
    steps_far = hop(steps_left[:cut], 2, 1), hop(steps_right[cut:], 2, -1)
    prompts_left, prompts_right = both(prompts_near, 2)
    cut = prompts_near.shape[0] // 2
    prompts_far = hop(prompts_left[:cut], 2, 1), hop(prompts_right[cut:], 2, -1)

    places = jnp.arange(CHIPS, dtype=jnp.int32)

    def offset_of(place):
        return jnp.where(place == 1, -1, jnp.where(place == 2, 1, jnp.where(place == 3, 2, 0)))

    inner, outer = offset_of(places % 4), offset_of(places // 4)
    by_core = (
        (x + inner) % X * Z + (z + outer) % Z,
        (x + outer) % X * Z + (z + inner) % Z,
    )
    tables = jnp.stack(
        [jnp.where(first_core, by_core[0], by_core[1]), jnp.where(first_core, by_core[1], by_core[0])]
    )

    groups = stretch_slot.reshape(POOLS, group_tokens)
    index = jnp.arange(group_tokens, dtype=jnp.int32)
    previous = jnp.concatenate([groups[:, :1] - 1, groups[:, :-1]], 1)
    opening = groups != previous
    rank = jnp.cumsum(opening.astype(jnp.int32), axis=1) - 1
    runs = jnp.arange(RUNS, dtype=jnp.int32)
    in_run = rank[:, None, :] == runs[None, :, None]
    run_counts = jnp.sum(in_run, axis=2, dtype=jnp.int32)
    run_slots = jnp.max(jnp.where(in_run, groups[:, None, :], -1), axis=2)
    run_begins = jnp.min(jnp.where(in_run, index[None, None, :], group_tokens), axis=2)
    here_slots = lax.dynamic_index_in_dim(groups, pool, 0, keepdims=False)
    here_rank = lax.dynamic_index_in_dim(rank, pool, 0, keepdims=False)
    here_begins = lax.dynamic_index_in_dim(run_begins, pool, 0, keepdims=False)
    here_runs = lax.dynamic_index_in_dim(run_slots, pool, 0, keepdims=False)
    here_counts = lax.dynamic_index_in_dim(run_counts, pool, 0, keepdims=False)
    hot = here_rank[:, None] == runs[None, :]
    positions = index - jnp.sum(jnp.where(hot, here_begins[None, :], 0), axis=1)
    prompt_tables = rope_tables(positions)
    step_index = jnp.repeat(jnp.arange(STEPS, dtype=jnp.int32), RUNS)
    compact_slots = jnp.tile(here_runs, STEPS)
    compact_tables = rope_tables(jnp.tile(here_counts, STEPS) + step_index)

    def place(slots, step):
        far_by = (slots // pool_slots - pool) % POOLS
        kept = jnp.where(far_by == 1, 2, jnp.where(far_by == 2, 3, jnp.where(far_by == 3, 1, 0)))
        row = kept * (pool_slots * STEPS) + row_of(slots % pool_slots, step, per_device)
        return jnp.where(slots < 0, -1, row)

    picks = place(compact_slots, step_index)[:, None]
    their_runs = jnp.concatenate(
        [lax.dynamic_slice_in_dim(run_slots, (pool + s) % POOLS, 1, 0) for s in OFFSETS], 0
    )
    their_runs = jnp.tile(their_runs, (1, STEPS))
    back = jnp.where(
        (their_runs >= 0) & (their_runs // pool_slots == pool),
        row_of(their_runs % pool_slots, step_index[None, :], per_device),
        -1,
    )
    my_slots = (pool * CHIPS * CORES + device) * per_device + jnp.arange(per_device, dtype=jnp.int32)
    counts = jnp.sum(stretch_slot[None, :] == my_slots[:, None], axis=1, dtype=jnp.int32)
    moments = jnp.arange(STEPS, dtype=jnp.int32)[:, None] + (cache_length + counts)[None, :]
    owner_tables = rope_tables(moments.reshape(-1))
    named = jnp.tile(counts, STEPS)[:, None]

    kept, got = partial_of([steps_near, steps_left, steps_right, *steps_far], steps_each)
    step_query, step_pair = assemble(tables, [kept], [got], width)
    step_query = step_query.reshape(CHIPS * CORES, step_rows, width)
    step_pair = step_pair.reshape(CHIPS * CORES, step_rows, -1)
    arrived = lax.all_to_all(
        jnp.concatenate([step_query, step_pair], 2), TP, split_axis=0, concat_axis=0, tiled=True
    )
    cached = cached_attention(arrived, cache_length, owner_tables, cache_keys, cache_values)

    def neighbour(kv):
        return lax.ppermute(kv, "z", [(k, k ^ 1) for k in range(Z)])

    flat = CHIPS * CORES * step_rows
    step_query, step_pair = step_query.reshape(flat, width), step_pair.reshape(flat, -1)
    step_flat = jnp.concatenate([step_query, step_pair, neighbour(step_pair)], 1)
    decode_rows = (step_flat, *pool_others(step_flat))

    parts = [
        partial_of([prompts_near], prompts_each),
        partial_of([prompts_left, prompts_right], prompts_each),
        partial_of([*prompts_far], prompts_each),
    ]
    queries, pair = assemble(tables, [p[0] for p in parts], [p[1] for p in parts], width)
    queries, pair = queries.reshape(group_tokens, -1), pair.reshape(group_tokens, -1)
    even, odd = pair, neighbour(pair)
    parity = (z % 2).astype(jnp.int32)[None]
    compact = prompt_slot_attention(
        parity,
        picks,
        compact_slots[:, None],
        decode_rows,
        even,
        odd,
        prompt_tables,
        compact_tables,
        here_slots[None, :],
    )
    prompt_out = prompt_attention(
        parity, queries, even, odd, prompt_tables, here_slots[:, None], here_slots[None, :]
    )
    ready = spread(back, (compact, *pool_others(compact)))
    ready = ready.reshape(CHIPS * CORES, step_rows, -1)
    prompted = lax.all_to_all(ready, TP, split_axis=0, concat_axis=0, tiled=True)
    step_out = merge(cached, prompted, named).reshape(STEPS, per_device, -1)
    return prompt_out, step_out


def solution(mesh):
    fine = Mesh(mesh.devices.reshape(POOLS, X, Z, CORES), ALL)
    in_specs = (
        P(ALL, None),
        P(),
        P(ALL),
        P(ALL, None, None),
        P(ALL, None, None),
        P(None, ALL, None),
        P(None, TP),
        P(None, TP),
        P(None, TP),
    )
    out_specs = (P("pool", TP), P(None, ALL, None))
    return jax.shard_map(
        on_device, mesh=fine, in_specs=in_specs, out_specs=out_specs, check_vma=False
    )
```
